32 devices in a mesh: dp: 16 (over z, y, core), tensor: 2 (over x).
Axes of the slice: x: 2, y: 2, z: 4, core: 2. Of those that a mesh axis runs over, the one named last changes fastest.
Arguments:
- activations: bfloat16 [32768, 1024], P(('dp', 'tensor')), may hold values from -6 to 6
- gradients: bfloat16 [32768, 5472], P('dp', 'tensor'), may hold values from -6 to 6
- act_history: float32 [2, 16, 1024], P('tensor'), may hold values from 0.1 to 4
- grad_history: float32 [16, 5472], P(None, 'tensor'), may hold values from 0.1 to 4
- owner_rank: int32 [1024], replicated, may hold values from 0 to 1
- history_slot: int32 [6496], replicated, may hold values from 0 to 15
Outputs:
- weight_grad: float32 [1024, 5472], P('dp', 'tensor')
- act_history_out: float32 [2, 16, 1024], P('tensor')
- grad_history_out: float32 [16, 5472], P(None, 'tensor')
The draws below stay inside these ranges and needn't reach their ends.
All inputs are finite; a program needn't handle non-finite values.
Results may differ from the reference program's by a relative error of at most 0.0042.
Values may be sent and summed in bfloat16 or wider, within the bound.
No kernel may reach another device: no remote copies, remote signals or barrier semaphores. Data moves between devices by JAX's collectives and lax.ppermute only.
A program may use at most 64 MiB of HBM per device.

```python
import math
import jax
import jax.numpy as jnp
from jax import lax

D = 1024
FF = 5472
HIST = 16
TOKENS = 32768
N_TENSOR = 2


def set_ends(values, own_key, least, high):
    longest = values.shape.index(max(values.shape))
    spots = []
    for shift in (0, 1):
        where = [jax.random.randint(jax.random.fold_in(own_key, axis), (), 0, length) for axis, length in enumerate(values.shape)]
        where[longest] = (where[longest] + shift) % values.shape[longest]
        spots.append(tuple(where))
    return values.at[spots[0]].set(least).at[spots[1]].set(high)


def with_spikes(values, own_key, source, target, shards_of, factor):
    owner, partner = [(jnp.arange(values.shape[dim]) // (values.shape[dim] // shards_of)).reshape([-1 if axis == dim else 1 for axis in range(values.ndim)]) for dim in (source, target)]
    chosen = jax.random.permutation(own_key, shards_of)[partner]
    strong = (owner == chosen) | (owner == (partner + shards_of // 2) % shards_of)
    return jnp.where(strong, factor * values, values)


def shard_levels(stream_key, shape, cuts, least, largest):
    def one(position, shards_of):
        draws = jax.random.uniform(jax.random.fold_in(jax.random.fold_in(stream_key, 6), position), (shards_of,), jnp.float32, least / len(cuts), largest / len(cuts))
        return jnp.repeat(jnp.exp(draws), shape[position] // shards_of).reshape((-1,) + (1,) * (len(shape) - position - 1))

    factor_of = one(*cuts[0])
    for cut in cuts[1:]:
        factor_of = factor_of * one(*cut)
    return factor_of


def gaussian(key, shape, width, limit, split=(), held_as=jnp.bfloat16):
    result = jax.random.normal(key, shape, jnp.float32) * width
    if len(split) > 0:
        result = shard_levels(key, shape, split, -0.22, 0.18) * result
    return jnp.clip(result, min=-limit, max=limit).astype(held_as)


def bell_draw_with(own_key, shape, deviation, most, split, heavy, held_as=jnp.bfloat16):
    result = deviation * jax.random.normal(own_key, shape, jnp.float32)
    if split:
        result = result * shard_levels(own_key, shape, split, -0.22, 0.18)
    return jnp.clip(with_spikes(result, jax.random.fold_in(own_key, 3), *heavy), -most, most).astype(held_as)


def setup_inputs(seed: int = 0) -> dict:
    splits = jax.random.split(jax.random.key(seed), 7)
    return {
        "activations": bell_draw_with(splits[0], (TOKENS, D), 1.0, 6.0, ((0, 32),), (0, 1, 32, 2.75)),
        "gradients": gaussian(splits[1], (TOKENS, FF), 1.0, 6.0, ((0, 16), (1, 2))),
        "act_history": jnp.clip(jnp.exp(math.log(4.0) - 3.6888794 * jax.random.uniform(splits[2], (N_TENSOR, HIST, D), jnp.float32) ** shard_levels(splits[2], (N_TENSOR, HIST, D), ((0, 2),), -0.2, 0.2)), 0.1, 4.0),
        "grad_history": jnp.clip(jnp.exp(math.log(4.0) - 3.6888794 * jax.random.uniform(splits[3], (HIST, FF), jnp.float32) ** shard_levels(splits[3], (HIST, FF), ((1, 2),), -0.2, 0.2)), 0.1, 4.0),
        "owner_rank": set_ends(jax.random.randint(splits[4], (D,), 0, N_TENSOR), jax.random.fold_in(splits[4], 1), 0, N_TENSOR - 1).astype(jnp.int32),
        "history_slot": set_ends(jax.random.randint(splits[5], (D + FF,), 0, HIST), jax.random.fold_in(splits[5], 1), 0, HIST - 1).astype(jnp.int32),
    }


QUANT_LIMIT = 448.0
SCALE_FLOOR = 0.25

def quantize(values, scale):
    scaled = values.astype(jnp.float32) * scale
    return jnp.clip(scaled, -QUANT_LIMIT, QUANT_LIMIT).astype(jnp.bfloat16)

def place_peaks(history, peaks, slots):
    rows = lax.broadcasted_iota(jnp.int32, history.shape, 0)
    return jnp.where(rows == slots.astype(jnp.int32)[None, :], peaks[None, :], history)

def reference(activations, gradients, act_history, grad_history, owner_rank, history_slot):
    ranks = lax.broadcasted_iota(jnp.int32, act_history.shape, 0)
    picked = jnp.where(ranks == owner_rank.astype(jnp.int32)[None, None, :], act_history, jnp.float32(0.0))
    current_history = lax.optimization_barrier(jnp.sum(picked, axis=0))
    act_scale = QUANT_LIMIT / jnp.maximum(lax.optimization_barrier(jnp.max(current_history, axis=0)), SCALE_FLOOR)
    grad_scale = QUANT_LIMIT / jnp.maximum(lax.optimization_barrier(jnp.max(grad_history, axis=0)), SCALE_FLOOR)
    act_quant = quantize(activations, act_scale)
    block_width = FF // 4
    results = []
    for block_index in range(4):
        first_col = block_index * block_width
        grad_block = quantize(gradients[:, first_col:first_col + block_width], grad_scale[first_col:first_col + block_width])
        results.append(jnp.dot(act_quant.T, grad_block, preferred_element_type=jnp.float32))
    summed = jnp.concatenate(results, axis=1)
    grad_factor = 1.0 / math.sqrt(TOKENS)
    weight_grad = summed / (act_scale[:, None] * grad_scale[None, :]) * grad_factor
    act_peak = lax.optimization_barrier(jnp.max(jnp.abs(activations), axis=0)).astype(jnp.float32)
    grad_peak = lax.optimization_barrier(jnp.max(jnp.abs(gradients), axis=0)).astype(jnp.float32)
    updated = place_peaks(current_history, act_peak, history_slot[:D])
    act_history_out = jnp.broadcast_to(updated[None], (N_TENSOR, HIST, D))
    grad_history_out = place_peaks(grad_history, grad_peak, history_slot[D:])
    return (weight_grad, act_history_out, grad_history_out)
```

```python
import math

import jax
import jax.numpy as jnp
from jax import lax
from jax.sharding import PartitionSpec as P

QUANT_LIMIT = 448.0
SCALE_FLOOR = 0.25


def quantize(values, scale):
    scaled = values.astype(jnp.float32) * scale
    return jnp.clip(scaled, -QUANT_LIMIT, QUANT_LIMIT).astype(jnp.bfloat16)


def place_peaks(history, peaks, slots):
    rows = lax.broadcasted_iota(jnp.int32, history.shape, 0)
    return jnp.where(rows == slots[None, :], peaks[None, :], history)


def shifted(values, axis, shift):
    size = lax.axis_size(axis)
    return lax.ppermute(values, axis, [(i, (i + shift) % size) for i in range(size)])


def butterfly_max(values, axis):
    size = lax.axis_size(axis)
    if size & (size - 1):
        return lax.pmax(values, axis)
    step = 1
    while step < size:
        other = lax.ppermute(values, axis, [(i, i ^ step) for i in range(size)])
        values = jnp.maximum(values, other)
        step *= 2
    return values


def after(values, *others):
    return lax.optimization_barrier((values,) + others)[0]


def peak_schedule(size, slots):
    steps = [1 << bit for bit in range(size.bit_length() - 1)]
    return [steps[len(steps) * k // slots : len(steps) * (k + 1) // slots] for k in range(slots)]


def body(activations, gradients, act_history, grad_history, owner_rank, history_slot):
    model_width = act_history.shape[2]
    token_rows = activations.shape[0]
    column_total = gradients.shape[1]
    tensor_size = lax.axis_size("tensor")
    dp_size = lax.axis_size("dp")
    my_rank = lax.axis_index("tensor")
    my_dp = lax.axis_index("dp")
    plane_count = dp_size // 4
    rows = model_width // dp_size
    plane_width = 4 * rows
    my_core = my_dp % 2
    my_y = (my_dp // 2) % 2
    my_plane = my_dp // 4
    grad_factor = 1.0 / math.sqrt(gradients.shape[0] * dp_size)

    planes = [(my_plane + 1 + k) % plane_count for k in range(plane_count)]

    def plane_of(values, plane, axis):
        return lax.dynamic_slice_in_dim(values, plane * plane_width, plane_width, axis)

    histories = [shifted(act_history[0], "tensor", shift) for shift in range(1, tensor_size)]
    pieces = [plane_of(activations, plane, 1) for plane in planes]
    received = [
        [shifted(piece, "tensor", shift) for shift in range(1, tensor_size)] for piece in pieces
    ]
    current_history = jnp.where(owner_rank[None, :] == my_rank, act_history[0], jnp.float32(0.0))
    for shift in range(1, tensor_size):
        source = (my_rank - shift) % tensor_size
        current_history = jnp.where(
            owner_rank[None, :] == source, histories[shift - 1], current_history
        )

    act_scale = QUANT_LIMIT / jnp.maximum(jnp.max(current_history, axis=0), SCALE_FLOOR)
    grad_scale = QUANT_LIMIT / jnp.maximum(jnp.max(grad_history, axis=0), SCALE_FLOOR)
    act_scale, grad_scale = lax.optimization_barrier((act_scale, grad_scale))

    def token_block(rank):
        block = lax.dynamic_slice_in_dim(gradients, rank * token_rows, token_rows, 0)
        return quantize(block, grad_scale)

    own_grad = token_block(my_rank)
    other_grad = jnp.concatenate(
        [token_block((my_rank - shift) % tensor_size) for shift in range(1, tensor_size)], axis=0
    )
    own_grad, other_grad = lax.optimization_barrier((own_grad, other_grad))
    contract_rows = (((0,), (0,)), ((), ()))

    def product(left, right):
        return lax.dot_general(left, right, contract_rows, preferred_element_type=jnp.float32)

    core_pairs = [(i, i ^ 1) for i in range(dp_size)]
    y_pairs = [(i, i ^ 2) for i in range(dp_size)]
    width = 2 * rows
    scales = [plane_of(act_scale, plane, 0) for plane in planes]
    own_parts = [
        product(quantize(piece, scale), own_grad) for piece, scale in zip(pieces, scales)
    ]

    def unit(k, remote, y_target):
        offset = y_target * width
        piece = lax.dynamic_slice_in_dim(remote, offset, width, 1)
        piece_scale = lax.dynamic_slice_in_dim(scales[k], offset, width, 0)
        part = product(quantize(piece, piece_scale), other_grad)
        part = part + lax.dynamic_slice_in_dim(own_parts[k], offset, width, 0)
        part = lax.optimization_barrier(part)
        away = lax.dynamic_slice_in_dim(part, (1 - my_core) * rows, rows, 0)
        away = lax.optimization_barrier(away.astype(jnp.bfloat16))
        kept = lax.dynamic_slice_in_dim(part, my_core * rows, rows, 0)
        return kept, away, lax.ppermute(away, "dp", core_pairs)

    def widen(values):
        return values.astype(jnp.float32)

    def plane_total(state):
        kept, landed, from_neighbour = state
        return kept + widen(landed) + widen(from_neighbour)

    def send_plane(k, total):
        hop = 4 * (k + 1)
        pairs = [(i, (i + hop) % dp_size) for i in range(dp_size)]
        return lax.ppermute(total, "dp", pairs)

    own_act_peak = jnp.max(jnp.abs(activations), axis=0).astype(jnp.float32)
    own_grad_peak = jnp.max(jnp.abs(after(gradients, own_grad)), axis=0).astype(jnp.float32)
    act_peak = butterfly_max(own_act_peak, "tensor")
    peaks = jnp.concatenate([act_peak, own_grad_peak])
    peak_steps = peak_schedule(dp_size, plane_count)

    arrivals = []
    state = None
    ready = ()
    for k in range(plane_count):
        remote = jnp.concatenate(received[k], axis=0) if tensor_size > 2 else received[k][0]
        remote = after(remote, *ready)
        kept_away, sent, landed_away = unit(k, remote, 1 - my_y)
        kept, sent, landed = unit(k, after(remote, sent), my_y)
        to_neighbour = (kept_away + widen(after(landed_away, sent))).astype(jnp.bfloat16)
        to_neighbour = lax.optimization_barrier(to_neighbour)
        from_neighbour = lax.ppermute(to_neighbour, "dp", y_pairs)
        ready = (to_neighbour,)
        if state is not None:
            kept_last, landed_last, from_last = state
            total = plane_total((kept_last, landed_last, after(from_last, to_neighbour)))
            total = lax.optimization_barrier(total.astype(jnp.bfloat16))
            arrivals.append(send_plane(k - 1, total))
            ready = (to_neighbour, total)
        state = (kept, landed, from_neighbour)
        for step in peak_steps[k]:
            peaks = after(peaks, to_neighbour)
            other = lax.ppermute(peaks, "dp", [(i, i ^ step) for i in range(dp_size)])
            peaks = jnp.maximum(peaks, other)
    summed = plane_total(state)
    for arrival in arrivals:
        summed = summed + widen(arrival)

    peaks, current_history, grad_history = lax.optimization_barrier(
        (peaks, current_history, grad_history)
    )
    act_peak = peaks[:model_width]
    grad_peak = peaks[model_width:]

    row_scale = lax.dynamic_slice_in_dim(act_scale, my_dp * rows, rows, 0)
    weight_grad = summed / (row_scale[:, None] * grad_scale[None, :]) * grad_factor
    act_slots = history_slot[:model_width]
    grad_slots = lax.dynamic_slice_in_dim(
        history_slot, model_width + my_rank * column_total, column_total, 0
    )
    act_history_out = place_peaks(current_history, act_peak, act_slots)[None]
    grad_history_out = place_peaks(grad_history, grad_peak, grad_slots)
    return (weight_grad, act_history_out, grad_history_out)


def solution(mesh):
    placed = (
        P(("dp", "tensor"), None),
        P("dp", "tensor"),
        P("tensor", None, None),
        P(None, "tensor"),
        P(),
        P(),
    )
    return jax.shard_map(
        body,
        mesh=mesh,
        in_specs=placed,
        out_specs=(P("dp", "tensor"), P("tensor", None, None), P(None, "tensor")),
        check_vma=False,
    )
```

```python
import math

import jax
import jax.numpy as jnp
from jax import lax
from jax.experimental.layout import Layout, with_layout_constraint
from jax.sharding import PartitionSpec as P

QUANT_LIMIT = 448.0
SCALE_FLOOR = 0.25


def quantize(values, scale):
    scaled = values.astype(jnp.float32) * scale
    return jnp.clip(scaled, -QUANT_LIMIT, QUANT_LIMIT).astype(jnp.bfloat16)


def place_peaks(history, peaks, slots):
    rows = lax.broadcasted_iota(jnp.int32, history.shape, 0)
    return jnp.where(rows == slots[None, :], peaks[None, :], history)


def shifted(values, axis, shift):
    size = lax.axis_size(axis)
    return lax.ppermute(values, axis, [(i, (i + shift) % size) for i in range(size)])


def butterfly_max(values, axis):
    size = lax.axis_size(axis)
    if size & (size - 1):
        return lax.pmax(values, axis)
    step = 1
    while step < size:
        other = lax.ppermute(values, axis, [(i, i ^ step) for i in range(size)])
        values = jnp.maximum(values, other)
        step *= 2
    return values


def after(values, *others):
    return lax.optimization_barrier((values,) + others)[0]


def row_major(values):
    return with_layout_constraint(values, Layout(major_to_minor=(0, 1)))


def body(activations, gradients, act_history, grad_history, owner_rank, history_slot):
    model_width = act_history.shape[2]
    token_rows = activations.shape[0]
    column_total = gradients.shape[1]
    tensor_size = lax.axis_size("tensor")
    dp_size = lax.axis_size("dp")
    my_rank = lax.axis_index("tensor")
    my_dp = lax.axis_index("dp")
    plane_count = dp_size // 4
    rows = model_width // dp_size
    plane_width = 4 * rows
    my_core = my_dp % 2
    my_y = (my_dp // 2) % 2
    my_plane = my_dp // 4
    grad_factor = 1.0 / math.sqrt(gradients.shape[0] * dp_size)

    planes = [(my_plane + 1 + k) % plane_count for k in range(plane_count)]

    def plane_of(values, plane, axis):
        return lax.dynamic_slice_in_dim(values, plane * plane_width, plane_width, axis)

    history = act_history[0]
    histories = [shifted(history, "tensor", shift) for shift in range(1, tensor_size)]
    pieces = [plane_of(activations, plane, 1) for plane in planes]
    received = []
    for piece in pieces:
        received.append([shifted(piece, "tensor", shift) for shift in range(1, tensor_size)])
    current_history = jnp.where(owner_rank[None, :] == my_rank, act_history[0], jnp.float32(0.0))
    for shift in range(1, tensor_size):
        source = (my_rank - shift) % tensor_size
        current_history = jnp.where(
            owner_rank[None, :] == source, histories[shift - 1], current_history
        )

    act_scale = QUANT_LIMIT / jnp.maximum(jnp.max(current_history, axis=0), SCALE_FLOOR)
    grad_scale = QUANT_LIMIT / jnp.maximum(jnp.max(grad_history, axis=0), SCALE_FLOOR)
    act_scale, grad_scale = lax.optimization_barrier((act_scale, grad_scale))

    def token_block(rank):
        block = lax.dynamic_slice_in_dim(gradients, rank * token_rows, token_rows, 0)
        return quantize(block, grad_scale)

    own_grad = token_block(my_rank)
    other_grad = jnp.concatenate(
        [token_block((my_rank - shift) % tensor_size) for shift in range(1, tensor_size)],
        axis=0,
    )
    own_grad, other_grad = lax.optimization_barrier((own_grad, other_grad))
    contract_rows = (((0,), (0,)), ((), ()))

    def product(left, right):
        result = lax.dot_general(left, right, contract_rows, preferred_element_type=jnp.float32)
        return row_major(result)

    core_pairs = [(i, i ^ 1) for i in range(dp_size)]
    y_pairs = [(i, i ^ 2) for i in range(dp_size)]
    scales = [plane_of(act_scale, plane, 0) for plane in planes]
    own_parts = []
    for k, piece in enumerate(pieces):
        own_part = product(quantize(piece, scales[k]), own_grad)
        own_parts.append(lax.optimization_barrier(own_part))

    def split(part):
        def block(y, core):
            return lax.dynamic_slice_in_dim(part, (2 * y + core) * rows, rows, 0)

        def exchange(y):
            away = row_major(block(y, 1 - my_core).astype(jnp.bfloat16))
            return lax.ppermute(lax.optimization_barrier(away), "dp", core_pairs)

        landed = (exchange(1 - my_y), exchange(my_y))

        def of(own_chip, *others):
            y = my_y if own_chip else 1 - my_y
            return block(y, my_core) + widen(after(landed[own_chip], *others))

        return of

    def widen(values):
        return values.astype(jnp.float32)

    def send_plane(k, total):
        hop = 4 * (k + 1)
        pairs = [(i, (i + hop) % dp_size) for i in range(dp_size)]
        return lax.ppermute(total, "dp", pairs)

    own_act_peak = jnp.max(jnp.abs(activations), axis=0)
    own_grad_peak = jnp.max(jnp.abs(after(gradients, own_grad)), axis=0)
    own_act_peak, own_grad_peak = lax.optimization_barrier((own_act_peak, own_grad_peak))
    own_act_peak = own_act_peak.astype(jnp.float32)
    own_grad_peak = own_grad_peak.astype(jnp.float32)
    peaks = jnp.concatenate([own_act_peak, own_grad_peak])
    peak_steps = [1 << bit for bit in range(dp_size.bit_length() - 1)]

    def partner_peaks(k, values):
        step = peak_steps[k]
        return lax.ppermute(values, "dp", [(i, i ^ step) for i in range(dp_size)])

    other_peaks = partner_peaks(0, peaks)
    peak_count = 1

    arrivals = []
    state = None
    ready = ()
    for k in range(plane_count):
        remote = jnp.concatenate(received[k], axis=0) if tensor_size > 2 else received[k][0]
        part = product(quantize(after(remote, *ready), scales[k]), other_grad) + own_parts[k]
        of = split(lax.optimization_barrier(part))
        to_neighbour = lax.optimization_barrier(row_major(of(False).astype(jnp.bfloat16)))
        from_neighbour = lax.ppermute(to_neighbour, "dp", y_pairs)
        ready = (to_neighbour,)
        if state is not None:
            of_last, from_last = state
            total = of_last(True) + widen(after(from_last, to_neighbour))
            total = lax.optimization_barrier(row_major(total.astype(jnp.bfloat16)))
            arrivals.append(send_plane(k - 1, total))
            ready = (to_neighbour, total)
        state = (of, from_neighbour)
        if peak_count < len(peak_steps):
            peaks = jnp.maximum(peaks, after(other_peaks, to_neighbour))
            other_peaks = partner_peaks(peak_count, peaks)
            peak_count += 1
    peaks = jnp.maximum(peaks, after(other_peaks, to_neighbour))
    while peak_count < len(peak_steps):
        peaks = jnp.maximum(peaks, partner_peaks(peak_count, peaks))
        peak_count += 1
    act_peak = butterfly_max(peaks[:model_width], "tensor")
    grad_peak = peaks[model_width:]
    of_last, from_last = state
    summed = of_last(True) + widen(from_last)
    for arrival in arrivals:
        summed = summed + widen(arrival)

    act_peak, grad_peak, current_history, grad_history = lax.optimization_barrier(
        (act_peak, grad_peak, current_history, grad_history)
    )

    row_scale = lax.dynamic_slice_in_dim(act_scale, my_dp * rows, rows, 0)
    weight_grad = summed / (row_scale[:, None] * grad_scale[None, :]) * grad_factor
    act_slots = history_slot[:model_width]
    grad_slots = lax.dynamic_slice_in_dim(
        history_slot, model_width + my_rank * column_total, column_total, 0
    )
    act_history_out = place_peaks(current_history, act_peak, act_slots)[None]
    grad_history_out = place_peaks(grad_history, grad_peak, grad_slots)
    return (weight_grad, act_history_out, grad_history_out)


def solution(mesh):
    placed = (
        P(("dp", "tensor"), None),
        P("dp", "tensor"),
        P("tensor", None, None),
        P(None, "tensor"),
        P(),
        P(),
    )

    return jax.shard_map(
        body,
        mesh=mesh,
        in_specs=placed,
        out_specs=(P("dp", "tensor"), P("tensor", None, None), P(None, "tensor")),
        check_vma=False,
    )
```

```python
import math

import jax
import jax.numpy as jnp
from jax import lax
from jax.experimental.layout import Layout, with_layout_constraint
from jax.sharding import PartitionSpec as P

QUANT_LIMIT = 448.0
SCALE_FLOOR = 0.25


def quantize(values, scale):
    scaled = values.astype(jnp.float32) * scale
    return jnp.clip(scaled, -QUANT_LIMIT, QUANT_LIMIT).astype(jnp.bfloat16)


def place_peaks(history, peaks, slots):
    rows = lax.broadcasted_iota(jnp.int32, history.shape, 0)
    return jnp.where(rows == slots[None, :], peaks[None, :], history)


def shifted(values, axis, shift):
    size = lax.axis_size(axis)
    return lax.ppermute(values, axis, [(i, (i + shift) % size) for i in range(size)])


def butterfly_max(values, axis):
    size = lax.axis_size(axis)
    if size & (size - 1):
        return lax.pmax(values, axis)
    step = 1
    while step < size:
        other = lax.ppermute(values, axis, [(i, i ^ step) for i in range(size)])
        values = jnp.maximum(values, other)
        step *= 2
    return values


def after(values, *others):
    return lax.optimization_barrier((values,) + others)[0]


def row_major(values):
    return with_layout_constraint(values, Layout(major_to_minor=(0, 1)))


def body(activations, gradients, act_history, grad_history, owner_rank, history_slot):
    model_width = act_history.shape[2]
    token_rows = activations.shape[0]
    column_total = gradients.shape[1]
    tensor_size = lax.axis_size("tensor")
    dp_size = lax.axis_size("dp")
    my_rank = lax.axis_index("tensor")
    my_dp = lax.axis_index("dp")
    plane_count = dp_size // 4
    rows = model_width // dp_size
    plane_width = 4 * rows
    my_core = my_dp % 2
    my_y = (my_dp // 2) % 2
    my_plane = my_dp // 4
    grad_factor = 1.0 / math.sqrt(gradients.shape[0] * dp_size)

    half = plane_count // 2
    hops = sorted(range(1, plane_count), key=lambda hop: abs(hop - half)) + [0]
    planes = [(my_plane + hop) % plane_count for hop in hops]

    def plane_of(values, plane, axis):
        return lax.dynamic_slice_in_dim(values, plane * plane_width, plane_width, axis)

    history = act_history[0]
    histories = [shifted(history, "tensor", shift) for shift in range(1, tensor_size)]
    pieces = [plane_of(activations, plane, 1) for plane in planes]
    received = []
    for piece in pieces:
        received.append([shifted(piece, "tensor", shift) for shift in range(1, tensor_size)])
    current_history = jnp.where(owner_rank[None, :] == my_rank, act_history[0], jnp.float32(0.0))
    for shift in range(1, tensor_size):
        source = (my_rank - shift) % tensor_size
        current_history = jnp.where(
            owner_rank[None, :] == source, histories[shift - 1], current_history
        )

    act_scale = QUANT_LIMIT / jnp.maximum(jnp.max(current_history, axis=0), SCALE_FLOOR)
    grad_scale = QUANT_LIMIT / jnp.maximum(jnp.max(grad_history, axis=0), SCALE_FLOOR)
    act_scale, grad_scale = lax.optimization_barrier((act_scale, grad_scale))

    def token_block(rank):
        block = lax.dynamic_slice_in_dim(gradients, rank * token_rows, token_rows, 0)
        return quantize(block, grad_scale)

    own_grad = token_block(my_rank)
    other_grad = jnp.concatenate(
        [token_block((my_rank - shift) % tensor_size) for shift in range(1, tensor_size)],
        axis=0,
    )
    own_grad, other_grad = lax.optimization_barrier((own_grad, other_grad))
    contract_rows = (((0,), (0,)), ((), ()))

    def product(left, right):
        result = lax.dot_general(left, right, contract_rows, preferred_element_type=jnp.float32)
        return row_major(result)

    core_pairs = [(i, i ^ 1) for i in range(dp_size)]
    y_pairs = [(i, i ^ 2) for i in range(dp_size)]
    scales = [plane_of(act_scale, plane, 0) for plane in planes]
    own_parts = []
    for k, piece in enumerate(pieces):
        own_part = product(quantize(piece, scales[k]), own_grad)
        own_parts.append(lax.optimization_barrier(own_part))

    def split(part):
        def block(y, core):
            return lax.dynamic_slice_in_dim(part, (2 * y + core) * rows, rows, 0)

        def exchange(y):
            away = row_major(block(y, 1 - my_core).astype(jnp.bfloat16))
            return lax.ppermute(lax.optimization_barrier(away), "dp", core_pairs)

        landed = (exchange(1 - my_y), exchange(my_y))

        def of(own_chip, *others):
            y = my_y if own_chip else 1 - my_y
            return block(y, my_core) + widen(after(landed[own_chip], *others))

        return of

    def widen(values):
        return values.astype(jnp.float32)

    def send_plane(k, total):
        pairs = [(i, (i + 4 * hops[k]) % dp_size) for i in range(dp_size)]
        return lax.ppermute(total, "dp", pairs)

    own_act_peak = jnp.max(jnp.abs(activations), axis=0)
    own_grad_peak = jnp.max(jnp.abs(after(gradients, own_grad)), axis=0)
    own_act_peak, own_grad_peak = lax.optimization_barrier((own_act_peak, own_grad_peak))
    own_act_peak = own_act_peak.astype(jnp.float32)
    own_grad_peak = own_grad_peak.astype(jnp.float32)
    peaks = jnp.concatenate([own_act_peak, own_grad_peak])
    peak_steps = [1 << bit for bit in reversed(range(dp_size.bit_length() - 1))]

    def partner_peaks(k, values):
        step = peak_steps[k]
        return lax.ppermute(values, "dp", [(i, i ^ step) for i in range(dp_size)])

    other_peaks = partner_peaks(0, peaks)
    peak_count = 1

    arrivals = []
    state = None
    ready = ()
    for k in range(plane_count):
        remote = jnp.concatenate(received[k], axis=0) if tensor_size > 2 else received[k][0]
        part = product(quantize(after(remote, *ready), scales[k]), other_grad) + own_parts[k]
        part = lax.optimization_barrier(part)
        of = split(part)
        total = None
        last = k + 1 == plane_count
        if last and state is not None:
            of_last, from_last = state
            total = of_last(True) + widen(after(from_last, part))
            total = lax.optimization_barrier(row_major(total.astype(jnp.bfloat16)))
            arrivals.append(send_plane(k - 1, total))
        to_neighbour = of(False, *(() if total is None else (total,)))
        to_neighbour = lax.optimization_barrier(row_major(to_neighbour.astype(jnp.bfloat16)))
        from_neighbour = lax.ppermute(to_neighbour, "dp", y_pairs)
        ready = (to_neighbour,)
        if state is not None and not last:
            of_last, from_last = state
            total = of_last(True) + widen(after(from_last, to_neighbour))
            total = lax.optimization_barrier(row_major(total.astype(jnp.bfloat16)))
            arrivals.append(send_plane(k - 1, total))
            ready = (to_neighbour, total)
        state = (of, from_neighbour)
        if peak_count < len(peak_steps):
            peaks = jnp.maximum(peaks, after(other_peaks, to_neighbour))
            other_peaks = partner_peaks(peak_count, peaks)
            peak_count += 1
    peaks = jnp.maximum(peaks, after(other_peaks, to_neighbour))
    while peak_count < len(peak_steps):
        peaks = jnp.maximum(peaks, partner_peaks(peak_count, peaks))
        peak_count += 1
    act_peak = butterfly_max(peaks[:model_width], "tensor")
    grad_peak = peaks[model_width:]
    of_last, from_last = state
    summed = of_last(True) + widen(from_last)
    for arrival in arrivals:
        summed = summed + widen(arrival)

    act_peak, grad_peak, current_history, grad_history = lax.optimization_barrier(
        (act_peak, grad_peak, current_history, grad_history)
    )

    row_scale = lax.dynamic_slice_in_dim(act_scale, my_dp * rows, rows, 0)
    weight_grad = summed / (row_scale[:, None] * grad_scale[None, :]) * grad_factor
    act_slots = history_slot[:model_width]
    grad_slots = lax.dynamic_slice_in_dim(
        history_slot, model_width + my_rank * column_total, column_total, 0
    )
    act_history_out = place_peaks(current_history, act_peak, act_slots)[None]
    grad_history_out = place_peaks(grad_history, grad_peak, grad_slots)
    return (weight_grad, act_history_out, grad_history_out)


def solution(mesh):
    placed = (
        P(("dp", "tensor"), None),
        P("dp", "tensor"),
        P("tensor", None, None),
        P(None, "tensor"),
        P(),
        P(),
    )

    return jax.shard_map(
        body,
        mesh=mesh,
        in_specs=placed,
        out_specs=(P("dp", "tensor"), P("tensor", None, None), P(None, "tensor")),
        check_vma=False,
    )
```
